256 devices in a mesh: bel: 64 (over z, x, y_lo), st: 4 (over y_hi, core).
Axes of the slice: x: 4, y: 4 (y_hi: 2, y_lo: 2; y = y_hi * 2 + y_lo), z: 8, core: 2. Of those that a mesh axis runs over, the one named last changes fastest.
Arguments:
- alphas: bfloat16 [512, 12288], P(None, 'st'), may hold values from -120 to 120
- transitions: bfloat16 [6, 12288, 12288], P(None, 'bel', 'st'), may hold values from 0.0009994507 to 10
- observe: bfloat16 [6, 48, 12288], P(None, None, 'st'), may hold values from 0.0019989014 to 0.19921875
- reward: bfloat16 [6, 12288], P(None, 'bel'), may hold values from -1.796875 to 1.796875
- belief_index: int32 [1024, 6, 48], P('bel'), may hold values from 0 to 511
- action: int32 [1024], replicated, may hold values from 0 to 5
Outputs:
- new_alphas: bfloat16 [1024, 12288], P('st', 'bel')
The draws below stay inside these ranges and needn't reach their ends.
Inputs may be any that keep to these rules, and one draw needn't show every extreme that they name: `belief_index`: indices of rows of alphas.
All inputs are finite; a program needn't handle non-finite values.
Results may differ from the reference program's by a relative error of at most 0.0044.
Values may be sent and summed in bfloat16 or wider, within the bound.
No kernel may reach another device: no remote copies, remote signals or barrier semaphores. Data moves between devices by JAX's collectives and lax.ppermute only.
A program may use at most 128 MiB of HBM per device.

```python
import math
import jax
import jax.numpy as jnp
from jax import lax

S = 12288
ACTS = 6
O = 48
K = 512
BELIEFS = 1024


def with_ends(values, rng, low, largest):
    index_at = [jax.random.randint(jax.random.fold_in(rng, axis), (), 0, length) for axis, length in enumerate(values.shape)]
    main_axis = values.shape.index(max(values.shape))
    neighbour = index_at[:main_axis] + [(index_at[main_axis] + 1) % values.shape[main_axis]] + index_at[main_axis + 1:]
    return values.at[tuple(index_at)].set(low).at[tuple(neighbour)].set(largest)


def block_scale(stream_key, extent, shards, smallest, high):
    loudness, own = 1.0, jax.random.fold_in(stream_key, 6)
    for dim, blocks in shards:
        heights = jnp.exp(jax.random.uniform(jax.random.fold_in(own, dim), (blocks,), jnp.float32, smallest / len(shards), high / len(shards)))
        loudness = loudness * jnp.repeat(heights, extent[dim] // blocks).reshape([-1 if axis == dim else 1 for axis in range(len(extent))])
    return loudness


def gaussian(stream_key, dims, width, most, shards=(), kind=jnp.bfloat16):
    drawn = jax.random.normal(stream_key, dims, jnp.float32) * width
    if len(shards) > 0:
        drawn = block_scale(stream_key, dims, shards, -0.22, 0.18) * drawn
    return jnp.clip(drawn, min=-most, max=most).astype(kind)


def setup_inputs(seed: int = 0) -> dict:
    seeds = jax.random.split(jax.random.key(seed), 7)
    alphas = gaussian(seeds[0], (K, S), 20.0, 120.0, ((1, 4),))
    transitions = jnp.clip(jnp.exp(math.log(10.0) - 9.21089 * jax.random.uniform(seeds[1], (ACTS, S, S), jnp.float32) ** block_scale(seeds[1], (ACTS, S, S), ((1, 64), (2, 4)), -0.2, 0.2)), 0.0009994507, 10.0).astype(jnp.bfloat16)
    observe = jnp.clip(jnp.exp(math.log(0.19921875) - 4.6018058 * jax.random.uniform(seeds[2], (ACTS, O, S), jnp.float32) ** block_scale(seeds[2], (ACTS, O, S), ((2, 4),), -0.2, 0.2)), 0.0019989014, 0.19921875).astype(jnp.bfloat16)
    reward = gaussian(seeds[3], (ACTS, S), 0.3, 1.796875, ((1, 64),))
    belief_index = with_ends(jax.random.randint(seeds[4], (BELIEFS, ACTS, O), 0, K), jax.random.fold_in(seeds[4], 1), 0, K - 1).astype(jnp.int32)
    action = with_ends(jax.random.randint(seeds[5], (BELIEFS,), 0, ACTS), jax.random.fold_in(seeds[5], 1), 0, ACTS - 1).astype(jnp.int32)
    return dict(alphas=alphas, transitions=transitions, observe=observe, reward=reward, belief_index=belief_index, action=action)


discount = 0.95


def mixture_block(alphas, observe, index_rows, action_rows):
    onehot = action_rows[:, None] == jnp.arange(ACTS, dtype=jnp.int32)[None, :]
    chosen = jnp.sum(jnp.where(onehot[:, :, None], index_rows, 0), axis=1).astype(jnp.int32)
    picked = alphas[chosen].astype(jnp.float32)
    weights = observe[action_rows].astype(jnp.float32)
    return jnp.sum(picked * weights, axis=1).astype(jnp.bfloat16)


def grouped_product(rows, acts, weights, block):
    count = rows.shape[0]
    kinds = weights.shape[0]
    blocks = count // block + kinds - 1
    onehot = (acts[:, None] == jnp.arange(kinds, dtype=jnp.int32)[None, :]).astype(jnp.int32)
    totals = jnp.sum(onehot, axis=0).astype(jnp.int32)
    filled = ((totals + block - 1) // block).astype(jnp.int32)
    ends = jnp.cumsum(filled).astype(jnp.int32)
    starts = (ends - filled).astype(jnp.int32)
    before = (jnp.cumsum(onehot, axis=0).astype(jnp.int32) - onehot).astype(jnp.int32)
    rank = jnp.sum(before * onehot, axis=1).astype(jnp.int32)
    first = jnp.sum(onehot * starts[None, :], axis=1).astype(jnp.int32)
    target = (first * block + rank).astype(jnp.int32)
    source = jnp.zeros((blocks * block,), jnp.int32).at[target].set(jnp.arange(count, dtype=jnp.int32))
    padded = rows[source].reshape(blocks, block, rows.shape[1])
    owner = jnp.sum((jnp.arange(blocks, dtype=jnp.int32)[:, None] >= ends[None, :]).astype(jnp.int32), axis=1)
    owner = jnp.minimum(owner, kinds - 1).astype(jnp.int32)

    def one_block(pair):
        part, which = pair
        matrix = lax.dynamic_index_in_dim(weights, which, 0, keepdims=False)
        return lax.dot_general(part, matrix, (((1,), (1,)), ((), ())), preferred_element_type=jnp.float32)

    result = lax.map(one_block, (padded, owner)).reshape(blocks * block, weights.shape[1])
    return result[target]


def reference(alphas, transitions, observe, reward, belief_index, action):
    beliefs = belief_index.shape[0]
    block = math.gcd(beliefs, 64)
    index_blocks = belief_index.reshape(beliefs // block, block, ACTS, O)
    action_blocks = action.reshape(beliefs // block, block)
    mixture = lax.map(lambda pair: mixture_block(alphas, observe, pair[0], pair[1]), (index_blocks, action_blocks))
    mixture = mixture.reshape(beliefs, S)
    carried = grouped_product(mixture, action, transitions, math.gcd(beliefs, 256))
    gained = reward[action].astype(jnp.float32)
    return (gained + (discount / S) * carried).astype(jnp.bfloat16)
```

```python
import functools

import jax
import jax.numpy as jnp
from jax import lax
from jax.experimental import pallas as pl
from jax.experimental.pallas import tpu as pltpu
from jax.sharding import Mesh
from jax.sharding import PartitionSpec as P

S = 12288
ACTS = 6
OBS = 48
ALPHAS = 512
BELIEFS = 1024
BEL = ("z", "x", "yl")
PEERS = 64
OWN = BELIEFS // PEERS
COLS = 3072
ROWS = 192
SUB = COLS // 128
CHUNK = 256
STEPS = BELIEFS // CHUNK
DISCOUNT = 0.95

NT = (((1,), (1,)), ((), ()))
NN = (((1,), (0,)), ((), ()))


def order_kernel(action_ref, index_ref, table_ref, sorted_ref, target_ref):
    act = action_ref[...]
    member = (lax.broadcasted_iota(jnp.int32, (8, BELIEFS), 0) == act).astype(jnp.float32)
    earlier = (
        lax.broadcasted_iota(jnp.int32, (BELIEFS, BELIEFS), 0)
        < lax.broadcasted_iota(jnp.int32, (BELIEFS, BELIEFS), 1)
    ).astype(jnp.float32).astype(jnp.bfloat16)
    before = lax.dot_general(member.astype(jnp.bfloat16), earlier, NN, preferred_element_type=jnp.float32)
    totals = jnp.sum(member, axis=1, keepdims=True)
    position = lax.broadcasted_iota(jnp.int32, (1, BELIEFS), 1)
    start = jnp.zeros((1, 1), jnp.float32)
    target = jnp.zeros((1, BELIEFS), jnp.float32)
    owner = jnp.zeros((1, BELIEFS), jnp.int32)
    for a in range(ACTS):
        target = target + member[a : a + 1] * (before[a : a + 1] + start)
        start = start + totals[a : a + 1]
        if a < ACTS - 1:
            owner = owner + (position >= start.astype(jnp.int32)).astype(jnp.int32)
    target = target.astype(jnp.int32)
    target_ref[...] = target
    sorted_ref[...] = owner
    index = index_ref[...]
    parts = jnp.concatenate([index >> 4, index & 15], axis=0).astype(jnp.float32).astype(jnp.bfloat16)
    for c in range(BELIEFS // 256):
        moved = (
            lax.broadcasted_iota(jnp.int32, (256, BELIEFS), 0) + c * 256 == target
        ).astype(jnp.float32).astype(jnp.bfloat16)
        got = lax.dot_general(parts, moved, NT, preferred_element_type=jnp.float32).astype(jnp.int32)
        table_ref[:, c * 256 : (c + 1) * 256] = (got[:OBS] * 16 + got[OBS:]) * SUB


def main_kernel(
    core_ref, table_ref, sorted_ref, owner_ref, target_ref, alphas_ref, observe_ref, weights_ref,
    keep_ref, send_ref, rows_ref, obs_ref, mix_ref, block_ref, terms_ref,
):
    step = pl.program_id(0)

    @pl.when(step == 0)
    def _():
        def spread(source, dest):
            def body(k, _):
                for j in range(SUB):
                    part = source[pl.ds(pl.multiple_of(k * 16, 16), 16), j * 128 : (j + 1) * 128]
                    dest[pl.ds(k * 16 * SUB + j, 16, stride=SUB), :] = part.astype(jnp.float32)
                return 0

            lax.fori_loop(0, source.shape[0] // 16, body, 0)

        spread(alphas_ref, rows_ref)
        spread(observe_ref, obs_ref)

    base = step * CHUNK

    def row(at):
        return rows_ref[pl.ds(pl.multiple_of(at, 8), SUB), :]

    def weight(at):
        return obs_ref[pl.ds(pl.multiple_of(at, 8), SUB), :]

    def sixteen(i, _):
        for half in range(2):
            first = i * 16 + half * 8
            a0 = sorted_ref[0, base + first]
            a1 = sorted_ref[0, base + first + 7]

            @pl.when(a0 == a1)
            def _():
                sums = [None] * 8
                for o in range(OBS):
                    w = weight((a0 * OBS + o) * SUB)
                    for r in range(8):
                        term = row(table_ref[o, first + r]) * w
                        sums[r] = term if o == 0 else sums[r] + term
                for r in range(8):
                    mix_ref[(half * 8 + r) * SUB : (half * 8 + r + 1) * SUB, :] = sums[r]

            @pl.when(a0 != a1)
            def _():
                def one(r, _):
                    a = sorted_ref[0, base + first + r]
                    total = None
                    for o in range(OBS):
                        term = row(table_ref[o, first + r]) * weight((a * OBS + o) * SUB)
                        total = term if o == 0 else total + term
                    mix_ref[pl.ds(pl.multiple_of((half * 8 + r) * SUB, 8), SUB), :] = total
                    return 0

                lax.fori_loop(0, 8, one, 0)

        for j in range(SUB):
            part = mix_ref[pl.ds(j, 16, stride=SUB), :]
            block_ref[pl.ds(pl.multiple_of(i * 16, 16), 16), j * 128 : (j + 1) * 128] = part.astype(jnp.bfloat16)
        return 0

    lax.fori_loop(0, CHUNK // 16, sixteen, 0)

    low = sorted_ref[0, base]
    high = sorted_ref[0, base + CHUNK - 1]
    here = pl.ds(pl.multiple_of(base, 128), CHUNK)
    owner = owner_ref[:, here]

    def three(t, _):
        a = jnp.minimum(low + 3 * t, ACTS - 3)
        matrix = weights_ref[pl.ds(pl.multiple_of(a * ROWS, 64), 3 * ROWS), :]
        got = lax.dot_general(matrix, block_ref[...], NT, preferred_element_type=jnp.float32)
        value = terms_ref[:, here]
        for d in range(3):
            value = jnp.where(owner == a + d, got[d * ROWS : (d + 1) * ROWS], value)
        terms_ref[:, here] = value
        return 0

    lax.fori_loop(0, (high - low) // 3 + 1, three, 0)

    @pl.when(step == STEPS - 1)
    def _():
        terms = terms_ref[...]
        big = terms.astype(jnp.bfloat16)
        small = (terms - big.astype(jnp.float32)).astype(jnp.bfloat16)
        both = jnp.concatenate([big, small], axis=0)
        core = core_ref[0]
        for ref, side in ((keep_ref, core), (send_ref, 1 - core)):
            for yh in range(2):
                at = pl.multiple_of((2 * yh + side) * 256, 128)
                moved = (
                    lax.broadcasted_iota(jnp.int32, (BELIEFS, 256), 0) == target_ref[:, pl.ds(at, 256)]
                ).astype(jnp.float32).astype(jnp.bfloat16)
                got = lax.dot_general(both, moved, NN, preferred_element_type=jnp.float32)
                ref[:, yh * 256 : (yh + 1) * 256] = got[:ROWS] + got[ROWS:]


def vmem():
    return pl.BlockSpec(memory_space=pltpu.VMEM)


def smem():
    return pl.BlockSpec(memory_space=pltpu.SMEM)


def body(alphas, transitions, observe, reward, belief_index, action):
    bel = lax.axis_index(BEL)
    core = lax.axis_index("co")
    high = lax.axis_index("yh")
    own_action = lax.dynamic_slice_in_dim(action, bel * OWN, OWN)
    onehot = own_action[:, None] == jnp.arange(ACTS, dtype=jnp.int32)[None, :]
    chosen = jnp.sum(jnp.where(onehot[:, :, None], belief_index, 0), axis=1)
    spread = jnp.broadcast_to(chosen[None], (PEERS, OWN, OBS))
    index = lax.all_to_all(spread, BEL, 0, 0, tiled=True)
    index = index.reshape(BELIEFS, OBS).T
    table, owner, target = pl.pallas_call(
        order_kernel,
        out_shape=(
            jax.ShapeDtypeStruct((OBS, BELIEFS), jnp.int32),
            jax.ShapeDtypeStruct((1, BELIEFS), jnp.int32),
            jax.ShapeDtypeStruct((1, BELIEFS), jnp.int32),
        ),
        in_specs=[vmem(), vmem()],
        out_specs=(vmem(), vmem(), vmem()),
        name="order",
    )(action.reshape(1, BELIEFS), index)
    keep, send = pl.pallas_call(
        main_kernel,
        grid=(STEPS,),
        out_shape=(
            jax.ShapeDtypeStruct((ROWS, 512), jnp.float32),
            jax.ShapeDtypeStruct((ROWS, 512), jnp.float32),
        ),
        in_specs=[
            smem(),
            pl.BlockSpec((OBS, CHUNK), lambda i: (0, i), memory_space=pltpu.SMEM),
            smem(),
            vmem(),
            vmem(),
            vmem(),
            vmem(),
            vmem(),
        ],
        out_specs=(vmem(), vmem()),
        scratch_shapes=[
            pltpu.VMEM((ALPHAS * SUB, 128), jnp.float32),
            pltpu.VMEM((ACTS * OBS * SUB, 128), jnp.float32),
            pltpu.VMEM((16 * SUB, 128), jnp.float32),
            pltpu.VMEM((CHUNK, COLS), jnp.bfloat16),
            pltpu.VMEM((ROWS, BELIEFS), jnp.float32),
        ],
        compiler_params=pltpu.CompilerParams(vmem_limit_bytes=50 * 2**20),
        name="mix",
    )(
        core.reshape(1),
        table,
        owner,
        owner,
        target,
        alphas,
        observe.reshape(ACTS * OBS, COLS),
        transitions.reshape(ACTS * ROWS, COLS),
    )
    across = [(0, 1), (1, 0)]
    half = keep + lax.ppermute(send, "co", across)
    mine = lax.dynamic_slice_in_dim(half, high * 256, 256, 1)
    theirs = lax.dynamic_slice_in_dim(half, (1 - high) * 256, 256, 1).astype(jnp.bfloat16)
    summed = mine + lax.ppermute(theirs, "yh", across).astype(jnp.float32)
    row_action = lax.dynamic_slice_in_dim(action, (2 * high + core) * 256, 256)
    picked = (row_action[:, None] == jnp.arange(ACTS, dtype=jnp.int32)[None, :]).astype(jnp.bfloat16)
    gained = jnp.dot(picked, reward, preferred_element_type=jnp.float32)
    return (gained + DISCOUNT / S * summed.T).astype(jnp.bfloat16)


def solution(mesh):
    torus = Mesh(mesh.devices.reshape(8, 4, 2, 2, 2), ("z", "x", "yl", "yh", "co"))
    st = ("yh", "co")
    in_specs = (
        P(None, st),
        P(None, BEL, st),
        P(None, None, st),
        P(None, BEL),
        P(BEL, None, None),
        P(),
    )
    return jax.shard_map(body, mesh=torus, in_specs=in_specs, out_specs=P(st, BEL), check_vma=False)
```

```python
import jax
import jax.numpy as jnp
from jax import lax
from jax.experimental import pallas as pl
from jax.experimental.pallas import tpu as pltpu
from jax.sharding import Mesh
from jax.sharding import PartitionSpec as P

S = 12288
ACTS = 6
OBS = 48
ALPHAS = 512
BELIEFS = 1024
BEL = ("z", "x", "yl")
PEERS = 64
OWN = BELIEFS // PEERS
COLS = 3072
ROWS = 192
HALF = COLS // 128
LINES = 2 * HALF
PITCH = 64
GAP = 56
PART = 256
DISCOUNT = 0.95

NT = (((1,), (1,)), ((), ()))


def prep_kernel(alphas_ref, alphas2_ref, observe_ref, observe2_ref, rows_ref, obs_ref, wide_ref):
    def spread(sources, dest):
        def body(k, _):
            at = pl.multiple_of(k * 16, 16)
            for s, source in enumerate(sources):
                for j in range(HALF):
                    part = source[pl.ds(at, 16), j * 128 : (j + 1) * 128]
                    wide_ref[pl.ds(s * HALF + j, 16, stride=GAP), :] = part.astype(jnp.float32)
            for r in range(16):
                dest[at + r, :LINES, :] = wide_ref[r * GAP : r * GAP + LINES, :].astype(jnp.bfloat16)
            return 0

        lax.fori_loop(0, sources[0].shape[0] // 16, body, 0)

    spread((alphas_ref, alphas2_ref), rows_ref)
    spread((observe_ref, observe2_ref), obs_ref)


def main_kernel(
    side_ref, index_ref, action_ref, owner_ref, rows_ref, obs_ref, here_ref, there_ref,
    send_ref, keep_ref, index_smem, weights_ref, mix_ref, block_ref, weight_sems, index_sem,
):
    fetch = [
        pltpu.make_async_copy(source, weights_ref.at[n], weight_sems.at[n])
        for n, source in enumerate((here_ref, there_ref))
    ]
    table = pltpu.make_async_copy(index_ref, index_smem, index_sem)
    table.start()
    for copy in fetch:
        copy.start()
    table.wait()
    high = side_ref[0]
    core = side_ref[1]

    for turn, out_ref in enumerate((send_ref, keep_ref)):
        yh = (1 - high) if turn == 0 else high
        block = 2 * yh + core

        def sixteen(i, _):
            source = block * 16 + i
            for h in range(2):
                for r in range(8):
                    a = action_ref[source * 16 + h * 8 + r]
                    total = None
                    for o in range(OBS):
                        k = index_smem[source, r, h * OBS + o]
                        term = rows_ref[k, :LINES, :].astype(jnp.float32) * obs_ref[a * OBS + o, :LINES, :].astype(jnp.float32)
                        total = term if o == 0 else total + term
                    mix_ref[(h * 8 + r) * GAP : (h * 8 + r) * GAP + LINES, :] = total
            for j in range(LINES):
                part = mix_ref[pl.ds(j, 16, stride=GAP), :]
                block_ref[j // HALF, pl.ds(pl.multiple_of(i * 16, 16), 16), (j % HALF) * 128 : (j % HALF + 1) * 128] = part.astype(jnp.bfloat16)
            return 0

        lax.fori_loop(0, PART // 16, sixteen, 0)
        if turn == 0:
            for copy in fetch:
                copy.wait()
        owner = owner_ref[:, pl.ds(pl.multiple_of(block * PART, 128), PART)]
        value = jnp.zeros((ROWS, PART), jnp.float32)
        for a in range(ACTS):
            got = sum(
                lax.dot_general(
                    weights_ref[n, a * ROWS : (a + 1) * ROWS, :], block_ref[n], NT, preferred_element_type=jnp.float32
                )
                for n in range(2)
            )
            value = jnp.where(owner == a, got, value)
        out_ref[...] = value.astype(out_ref.dtype)


def vmem():
    return pl.BlockSpec(memory_space=pltpu.VMEM)


def smem():
    return pl.BlockSpec(memory_space=pltpu.SMEM)


def anyspace():
    return pl.BlockSpec(memory_space=pl.ANY)


def body(alphas, transitions, observe, reward, belief_index, action):
    bel = lax.axis_index(BEL)
    core = lax.axis_index("co")
    high = lax.axis_index("yh")
    across = [(0, 1), (1, 0)]
    observe = observe.reshape(ACTS * OBS, COLS)
    transitions = transitions.reshape(ACTS * ROWS, COLS)
    alphas2, observe2, transitions2 = (lax.ppermute(v, "co", across) for v in (alphas, observe, transitions))
    own_action = lax.dynamic_slice_in_dim(action, bel * OWN, OWN)
    onehot = own_action[:, None] == jnp.arange(ACTS, dtype=jnp.int32)[None, :]
    chosen = jnp.sum(jnp.where(onehot[:, :, None], belief_index, 0), axis=1)
    packed = jnp.concatenate([chosen[:8], chosen[8:], jnp.zeros((8, 32), jnp.int32)], axis=1)
    index = lax.all_to_all(jnp.tile(packed, (PEERS, 1)), BEL, 0, 0, tiled=True)
    rows, obs = pl.pallas_call(
        prep_kernel,
        out_shape=(
            jax.ShapeDtypeStruct((ALPHAS, PITCH, 128), jnp.bfloat16),
            jax.ShapeDtypeStruct((ACTS * OBS, LINES, 128), jnp.bfloat16),
        ),
        in_specs=[vmem()] * 4,
        out_specs=(vmem(),) * 2,
        scratch_shapes=[pltpu.VMEM((16 * GAP, 128), jnp.float32)],
        compiler_params=pltpu.CompilerParams(vmem_limit_bytes=24 * 2**20),
        cost_estimate=pl.CostEstimate(flops=8 * 10**9, bytes_accessed=10**7, transcendentals=0),
        name="prep",
    )(alphas, alphas2, observe, observe2)
    send, keep = pl.pallas_call(
        main_kernel,
        out_shape=(
            jax.ShapeDtypeStruct((ROWS, PART), jnp.bfloat16),
            jax.ShapeDtypeStruct((ROWS, PART), jnp.float32),
        ),
        in_specs=[smem(), vmem(), smem(), vmem(), vmem(), vmem(), anyspace(), anyspace()],
        out_specs=(vmem(), vmem()),
        scratch_shapes=[
            pltpu.SMEM((PEERS, 8, 128), jnp.int32),
            pltpu.VMEM((2, ACTS * ROWS, COLS), jnp.bfloat16),
            pltpu.VMEM((16 * GAP, 128), jnp.float32),
            pltpu.VMEM((2, PART, COLS), jnp.bfloat16),
            pltpu.SemaphoreType.DMA((2,)),
            pltpu.SemaphoreType.DMA,
        ],
        compiler_params=pltpu.CompilerParams(vmem_limit_bytes=40 * 2**20),
        name="mix",
    )(
        jnp.stack([high, core]),
        index.reshape(PEERS, 8, 128),
        action,
        action.reshape(1, BELIEFS),
        rows,
        obs,
        transitions,
        transitions2,
    )
    summed = keep + lax.ppermute(send, "yh", across).astype(jnp.float32)
    row_action = lax.dynamic_slice_in_dim(action, (2 * high + core) * PART, PART)
    picked = (row_action[:, None] == jnp.arange(ACTS, dtype=jnp.int32)[None, :]).astype(jnp.bfloat16)
    gained = jnp.dot(picked, reward, preferred_element_type=jnp.float32)
    return (gained + DISCOUNT / S * summed.T).astype(jnp.bfloat16)


def solution(mesh):
    torus = Mesh(mesh.devices.reshape(8, 4, 2, 2, 2), ("z", "x", "yl", "yh", "co"))
    st = ("yh", "co")
    in_specs = (
        P(None, st),
        P(None, BEL, st),
        P(None, None, st),
        P(None, BEL),
        P(BEL, None, None),
        P(),
    )
    return jax.shard_map(body, mesh=torus, in_specs=in_specs, out_specs=P(st, BEL), check_vma=False)
```

```python
import jax
import jax.numpy as jnp
from jax import lax
from jax.experimental import pallas as pl
from jax.experimental.pallas import tpu as pltpu
from jax.sharding import Mesh
from jax.sharding import PartitionSpec as P

S = 12288
ACTS = 6
OBS = 48
ALPHAS = 512
BELIEFS = 1024
BEL = ("z", "x", "yl")
PEERS = 64
OWN = BELIEFS // PEERS
COLS = 3072
ROWS = 192
HALF = COLS // 128
LINES = 2 * HALF
PITCH = 64
GAP = 56
PART = 256
WEIGHTS = ALPHAS * PITCH
TOTAL = WEIGHTS + ACTS * OBS * LINES
STAGE = 32
DISCOUNT = 0.95

NT = (((1,), (1,)), ((), ()))


def prep_kernel(alphas_ref, alphas2_ref, observe_ref, observe2_ref, lines_ref, stage_ref, wide_ref, sems):
    counts = [ALPHAS // STAGE, ACTS * OBS // STAGE]

    def spread(sources, steps, first, pitch):
        def copies(t, slot):
            return [
                pltpu.make_async_copy(
                    source.at[pl.ds(pl.multiple_of(t * STAGE, STAGE), STAGE), :], stage_ref.at[slot, s], sems.at[slot, s]
                )
                for s, source in enumerate(sources)
            ]

        for slot in range(3):
            for copy in copies(slot, slot):
                copy.start()

        def step(t, _):
            slot = lax.rem(t, 4)

            @pl.when(t + 3 < steps)
            def _():
                for copy in copies(t + 3, lax.rem(t + 3, 4)):
                    copy.start()

            for copy in copies(t, slot):
                copy.wait()
            for g in range(STAGE // 16):
                for s in range(2):
                    for j in range(HALF):
                        part = stage_ref[slot, s, g * 16 : (g + 1) * 16, j * 128 : (j + 1) * 128]
                        wide_ref[pl.ds(s * HALF + j, 16, stride=GAP), :] = part.astype(jnp.float32)
                for r in range(16):
                    at = pl.multiple_of(first + (t * STAGE + g * 16 + r) * pitch, 16)
                    lines_ref[pl.ds(at, LINES), :] = wide_ref[r * GAP : r * GAP + LINES, :].astype(jnp.bfloat16)
            return 0

        lax.fori_loop(0, steps, step, 0)

    spread((alphas_ref, alphas2_ref), counts[0], 0, PITCH)
    spread((observe_ref, observe2_ref), counts[1], WEIGHTS, LINES)


def main_kernel(
    side_ref, index_ref, action_ref, owner_ref, source_ref, here_ref, there_ref,
    send_ref, keep_ref, lines_ref, index_smem, weights_ref, mix_ref, block_ref, weight_sems, index_sem, lines_sem,
):
    fetch = [
        pltpu.make_async_copy(source, weights_ref.at[n], weight_sems.at[n])
        for n, source in enumerate((here_ref, there_ref))
    ]
    table = pltpu.make_async_copy(index_ref, index_smem, index_sem)
    lines = pltpu.make_async_copy(source_ref, lines_ref, lines_sem)
    lines.start()
    table.start()
    for copy in fetch:
        copy.start()
    table.wait()
    lines.wait()
    rows_ref = lines_ref.at[pl.ds(0, WEIGHTS), :].reshape(ALPHAS, PITCH, 128)
    obs_ref = lines_ref.at[pl.ds(WEIGHTS, ACTS * OBS * LINES), :].reshape(ACTS * OBS, LINES, 128)
    high = side_ref[0]
    core = side_ref[1]

    def turn(t, _):
        block = 2 * jnp.where(t == 0, 1 - high, high) + core

        def sixteen(i, _):
            source = block * 16 + i
            for h in range(2):
                for r in range(8):
                    a = action_ref[source * 16 + h * 8 + r]
                    total = None
                    for o in range(OBS):
                        k = index_smem[source, r, h * OBS + o]
                        term = rows_ref[k, :LINES, :].astype(jnp.float32) * obs_ref[a * OBS + o].astype(jnp.float32)
                        total = term if o == 0 else total + term
                    mix_ref[(h * 8 + r) * GAP : (h * 8 + r) * GAP + LINES, :] = total
            for j in range(LINES):
                part = mix_ref[pl.ds(j, 16, stride=GAP), :]
                block_ref[j // HALF, pl.ds(pl.multiple_of(i * 16, 16), 16), (j % HALF) * 128 : (j % HALF + 1) * 128] = part.astype(jnp.bfloat16)
            return 0

        lax.fori_loop(0, PART // 16, sixteen, 0)

        @pl.when(t == 0)
        def _():
            for copy in fetch:
                copy.wait()

        got = lax.dot_general(weights_ref[0], block_ref[0], NT, preferred_element_type=jnp.float32)
        got += lax.dot_general(weights_ref[1], block_ref[1], NT, preferred_element_type=jnp.float32)
        owner = owner_ref[:, pl.ds(pl.multiple_of(block * PART, 128), PART)]
        value = got[:ROWS]
        for a in range(1, ACTS):
            value = jnp.where(owner == a, got[a * ROWS : (a + 1) * ROWS], value)

        @pl.when(t == 0)
        def _():
            send_ref[...] = value.astype(send_ref.dtype)

        @pl.when(t == 1)
        def _():
            keep_ref[...] = value

        return 0

    lax.fori_loop(0, 2, turn, 0)


def vmem():
    return pl.BlockSpec(memory_space=pltpu.VMEM)


def smem():
    return pl.BlockSpec(memory_space=pltpu.SMEM)


def hbm():
    return pl.BlockSpec(memory_space=pltpu.HBM)


def body(alphas, transitions, observe, reward, belief_index, action):
    bel = lax.axis_index(BEL)
    core = lax.axis_index("co")
    high = lax.axis_index("yh")
    across = [(0, 1), (1, 0)]
    observe = observe.reshape(ACTS * OBS, COLS)
    transitions = transitions.reshape(ACTS * ROWS, COLS)
    alphas2, observe2 = (lax.ppermute(v, "co", across) for v in (alphas, observe))
    own_action = lax.dynamic_slice_in_dim(action, bel * OWN, OWN)
    onehot = own_action[:, None] == jnp.arange(ACTS, dtype=jnp.int32)[None, :]
    chosen = jnp.sum(jnp.where(onehot[:, :, None], belief_index, 0), axis=1)
    packed = jnp.concatenate([chosen[:8], chosen[8:], jnp.zeros((8, 32), jnp.int32)], axis=1)
    late, packed = lax.optimization_barrier((transitions, packed))
    transitions2 = lax.ppermute(late, "co", across)
    index = lax.all_to_all(jnp.tile(packed, (PEERS, 1)), BEL, 0, 0, tiled=True)
    lines = pl.pallas_call(
        prep_kernel,
        out_shape=jax.ShapeDtypeStruct((TOTAL, 128), jnp.bfloat16),
        in_specs=[hbm()] * 4,
        out_specs=vmem(),
        scratch_shapes=[
            pltpu.VMEM((4, 2, STAGE, COLS), jnp.bfloat16),
            pltpu.VMEM((16 * GAP, 128), jnp.float32),
            pltpu.SemaphoreType.DMA((4, 2)),
        ],
        compiler_params=pltpu.CompilerParams(vmem_limit_bytes=62 * 2**20),
        cost_estimate=pl.CostEstimate(flops=8 * 10**9, bytes_accessed=10**7, transcendentals=0),
        name="prep",
    )(alphas, alphas2, observe, observe2)
    send, keep = pl.pallas_call(
        main_kernel,
        out_shape=(
            jax.ShapeDtypeStruct((ROWS, PART), jnp.bfloat16),
            jax.ShapeDtypeStruct((ROWS, PART), jnp.float32),
        ),
        in_specs=[smem(), vmem(), smem(), vmem(), hbm(), hbm(), hbm()],
        out_specs=(vmem(), vmem()),
        scratch_shapes=[
            pltpu.VMEM((TOTAL, 128), jnp.bfloat16),
            pltpu.SMEM((PEERS, 8, 128), jnp.int32),
            pltpu.VMEM((2, ACTS * ROWS, COLS), jnp.bfloat16),
            pltpu.VMEM((16 * GAP, 128), jnp.float32),
            pltpu.VMEM((2, PART, COLS), jnp.bfloat16),
            pltpu.SemaphoreType.DMA((2,)),
            pltpu.SemaphoreType.DMA,
            pltpu.SemaphoreType.DMA,
        ],
        compiler_params=pltpu.CompilerParams(vmem_limit_bytes=62 * 2**20),
        name="mix",
    )(
        jnp.stack([high, core]),
        index.reshape(PEERS, 8, 128),
        action,
        action.reshape(1, BELIEFS),
        lines,
        transitions,
        transitions2,
    )
    summed = keep + lax.ppermute(send, "yh", across).astype(jnp.float32)
    row_action = lax.dynamic_slice_in_dim(action, (2 * high + core) * PART, PART)
    picked = (row_action[:, None] == jnp.arange(ACTS, dtype=jnp.int32)[None, :]).astype(jnp.bfloat16)
    gained = jnp.dot(picked, reward, preferred_element_type=jnp.float32)
    return (gained + DISCOUNT / S * summed.T).astype(jnp.bfloat16)


def solution(mesh):
    torus = Mesh(mesh.devices.reshape(8, 4, 2, 2, 2), ("z", "x", "yl", "yh", "co"))
    st = ("yh", "co")
    in_specs = (
        P(None, st),
        P(None, BEL, st),
        P(None, None, st),
        P(None, BEL),
        P(BEL, None, None),
        P(),
    )
    return jax.shard_map(body, mesh=torus, in_specs=in_specs, out_specs=P(st, BEL), check_vma=False)
```

```python
import jax
import jax.numpy as jnp
from jax import lax
from jax.experimental import pallas as pl
from jax.experimental.pallas import tpu as pltpu
from jax.sharding import Mesh
from jax.sharding import PartitionSpec as P

S = 12288
ACTS = 6
OBS = 48
ALPHAS = 512
BELIEFS = 1024
BEL = ("z", "x", "yl")
PEERS = 64
OWN = BELIEFS // PEERS
COLS = 3072
ROWS = 192
HALF = COLS // 128
LINES = 2 * HALF
PITCH = 64
GAP = 56
PART = 256
WEIGHTS = ALPHAS * PITCH
TOTAL = WEIGHTS + ACTS * OBS * LINES
STAGE = 32
DISCOUNT = 0.95

NT = (((1,), (1,)), ((), ()))


def choose_kernel(index_ref, action_ref, out_ref, row_ref):
    bel = (lax.axis_index("z") * 4 + lax.axis_index("x")) * 2 + lax.axis_index("yl")
    row_ref[...] = jnp.zeros_like(row_ref)
    for r in range(OWN):
        row_ref[r : r + 1, :OBS] = index_ref[action_ref[bel * OWN + r], r : r + 1, :]
    packed = row_ref[:8] + pltpu.roll(row_ref[8:], 64, axis=1)
    out_ref[...] = jnp.broadcast_to(packed[None], (PEERS, 8, 128))


def prep_kernel(alphas_ref, alphas2_ref, observe_ref, observe2_ref, lines_ref, stage_ref, wide_ref, out_ref, sems, out_sems):
    def spread(sources, steps, first, pitch):
        def copies(t, slot):
            return [
                pltpu.make_async_copy(
                    source.at[pl.ds(pl.multiple_of(t * STAGE, STAGE), STAGE), :], stage_ref.at[slot, s], sems.at[slot, s]
                )
                for s, source in enumerate(sources)
            ]

        def result(t, slot):
            at = pl.multiple_of(first + t * STAGE * pitch, 16)
            return pltpu.make_async_copy(
                out_ref.at[slot, pl.ds(0, STAGE * pitch), :], lines_ref.at[pl.ds(at, STAGE * pitch), :], out_sems.at[slot]
            )

        for slot in range(3):
            for copy in copies(slot, slot):
                copy.start()

        def step(t, _):
            slot = lax.rem(t, 4)
            side = lax.rem(t, 2)

            @pl.when(t + 3 < steps)
            def _():
                for copy in copies(t + 3, lax.rem(t + 3, 4)):
                    copy.start()

            for copy in copies(t, slot):
                copy.wait()

            @pl.when(t >= 2)
            def _():
                result(t - 2, side).wait()

            for g in range(STAGE // 16):
                for s in range(2):
                    for j in range(HALF):
                        part = stage_ref[slot, s, g * 16 : (g + 1) * 16, j * 128 : (j + 1) * 128]
                        wide_ref[g, pl.ds(s * HALF + j, 16, stride=GAP), :] = part.astype(jnp.float32)
                for r in range(16):
                    at = (g * 16 + r) * pitch
                    out_ref[side, at : at + LINES, :] = wide_ref[g, r * GAP : r * GAP + LINES, :].astype(jnp.bfloat16)
            result(t, side).start()
            return 0

        lax.fori_loop(0, steps, step, 0)
        for t in (steps - 2, steps - 1):
            result(t, t % 2).wait()

    spread((alphas_ref, alphas2_ref), ALPHAS // STAGE, 0, PITCH)
    spread((observe_ref, observe2_ref), ACTS * OBS // STAGE, WEIGHTS, LINES)


def pick(owner, got):
    value = got[:ROWS]
    for a in range(1, ACTS):
        value = jnp.where(owner == a, got[a * ROWS : (a + 1) * ROWS], value)
    return value


def main_kernel(
    index_ref, action_ref, owner_ref, source_ref, here_ref, there_ref,
    send_ref, mixed_ref, lines_ref, index_smem, weights_ref, mix_ref, block_ref, weight_sems, index_sem, lines_sem, mixed_sem,
):
    fetch = [
        pltpu.make_async_copy(source, weights_ref.at[n], weight_sems.at[n])
        for n, source in enumerate((here_ref, there_ref))
    ]
    lines = pltpu.make_async_copy(source_ref, lines_ref, lines_sem)
    table = pltpu.make_async_copy(index_ref, index_smem, index_sem)
    lines.start()
    table.start()
    for copy in fetch:
        copy.start()
    table.wait()
    lines.wait()
    rows_ref = lines_ref.at[pl.ds(0, WEIGHTS), :].reshape(ALPHAS, PITCH, 128)
    obs_ref = lines_ref.at[pl.ds(WEIGHTS, ACTS * OBS * LINES), :].reshape(ACTS * OBS, LINES, 128)
    high = lax.axis_index("yh")
    core = lax.axis_index("co")

    def sixteen(n, _):
        t = n // 16
        i = lax.rem(n, 16)
        source = (2 * jnp.where(t == 0, 1 - high, high) + core) * 16 + i
        for h in range(2):
            for r in range(8):
                a = action_ref[source * 16 + h * 8 + r]
                own = index_smem.at[source, r]
                weight = obs_ref.at[pl.ds(a * OBS, OBS)]
                total = None
                for o in range(OBS):
                    term = rows_ref[own[h * 64 + o], :LINES, :].astype(jnp.float32) * weight[o].astype(jnp.float32)
                    total = term if o == 0 else total + term
                mix_ref[(h * 8 + r) * GAP : (h * 8 + r) * GAP + LINES, :] = total
        for j in range(LINES):
            part = mix_ref[pl.ds(j, 16, stride=GAP), :]
            at = pl.ds(pl.multiple_of(i * 16, 16), 16)
            block_ref[t, j // HALF, at, (j % HALF) * 128 : (j % HALF + 1) * 128] = part.astype(jnp.bfloat16)
        return 0

    lax.fori_loop(0, 2 * PART // 16, sixteen, 0)
    mixed = pltpu.make_async_copy(block_ref.at[1], mixed_ref, mixed_sem)
    mixed.start()
    for copy in fetch:
        copy.wait()
    got = lax.dot_general(weights_ref[0], block_ref[0, 0], NT, preferred_element_type=jnp.float32)
    got += lax.dot_general(weights_ref[1], block_ref[0, 1], NT, preferred_element_type=jnp.float32)
    first = pl.multiple_of((2 * (1 - high) + core) * PART, 128)
    send_ref[...] = pick(owner_ref[:, pl.ds(first, PART)], got).astype(send_ref.dtype)
    mixed.wait()


def rest_kernel(owner_ref, mixed_ref, here_ref, there_ref, keep_ref, sum_ref):
    step = pl.program_id(0)
    got = lax.dot_general(here_ref[...], mixed_ref[0], NT, preferred_element_type=jnp.float32)
    got += lax.dot_general(there_ref[...], mixed_ref[1], NT, preferred_element_type=jnp.float32)

    @pl.when(step == 0)
    def _():
        sum_ref[...] = got

    @pl.when(step > 0)
    def _():
        sum_ref[...] += got

    @pl.when(step == pl.num_programs(0) - 1)
    def _():
        first = pl.multiple_of((2 * lax.axis_index("yh") + lax.axis_index("co")) * PART, 128)
        keep_ref[...] = pick(owner_ref[:, pl.ds(first, PART)], sum_ref[...])


def vmem():
    return pl.BlockSpec(memory_space=pltpu.VMEM)


def smem():
    return pl.BlockSpec(memory_space=pltpu.SMEM)


def hbm():
    return pl.BlockSpec(memory_space=pltpu.HBM)


def gather_blocks(packed):
    return lax.all_to_all(packed, BEL, 0, 0, tiled=True)


def body(alphas, transitions, observe, reward, belief_index, action):
    core = lax.axis_index("co")
    high = lax.axis_index("yh")
    across = [(0, 1), (1, 0)]
    observe = observe.reshape(ACTS * OBS, COLS)
    transitions = transitions.reshape(ACTS * ROWS, COLS)
    alphas2 = lax.ppermute(alphas, "co", across)
    observe2 = lax.ppermute(observe, "co", across)
    packed = pl.pallas_call(
        choose_kernel,
        out_shape=jax.ShapeDtypeStruct((PEERS, 8, 128), jnp.int32),
        in_specs=[vmem(), smem()],
        out_specs=vmem(),
        scratch_shapes=[pltpu.VMEM((OWN, 128), jnp.int32)],
        name="choose",
    )(belief_index.transpose(1, 0, 2), action)
    index = gather_blocks(packed)
    transitions2 = lax.ppermute(transitions, "co", across)
    lines = pl.pallas_call(
        prep_kernel,
        out_shape=jax.ShapeDtypeStruct((TOTAL, 128), jnp.bfloat16),
        in_specs=[hbm()] * 4,
        out_specs=hbm(),
        scratch_shapes=[
            pltpu.VMEM((4, 2, STAGE, COLS), jnp.bfloat16),
            pltpu.VMEM((STAGE // 16, 16 * GAP, 128), jnp.float32),
            pltpu.VMEM((2, STAGE * PITCH, 128), jnp.bfloat16),
            pltpu.SemaphoreType.DMA((4, 2)),
            pltpu.SemaphoreType.DMA((2,)),
        ],
        compiler_params=pltpu.CompilerParams(vmem_limit_bytes=62 * 2**20),
        cost_estimate=pl.CostEstimate(flops=8 * 10**9, bytes_accessed=10**7, transcendentals=0),
        name="prep",
    )(alphas, alphas2, observe, observe2)
    owner = action.reshape(1, BELIEFS)
    send, mixed = pl.pallas_call(
        main_kernel,
        out_shape=(
            jax.ShapeDtypeStruct((ROWS, PART), jnp.bfloat16),
            jax.ShapeDtypeStruct((2, PART, COLS), jnp.bfloat16),
        ),
        in_specs=[vmem(), smem(), vmem(), hbm(), hbm(), hbm()],
        out_specs=(vmem(), hbm()),
        scratch_shapes=[
            pltpu.VMEM((TOTAL, 128), jnp.bfloat16),
            pltpu.SMEM((PEERS, 8, 128), jnp.int32),
            pltpu.VMEM((2, ACTS * ROWS, COLS), jnp.bfloat16),
            pltpu.VMEM((16 * GAP, 128), jnp.float32),
            pltpu.VMEM((2, 2, PART, COLS), jnp.bfloat16),
            pltpu.SemaphoreType.DMA((2,)),
            pltpu.SemaphoreType.DMA,
            pltpu.SemaphoreType.DMA,
            pltpu.SemaphoreType.DMA,
        ],
        compiler_params=pltpu.CompilerParams(vmem_limit_bytes=62 * 2**20),
        name="mix",
    )(index, action, owner, lines, transitions, transitions2)
    got = lax.ppermute(send, "yh", across)
    wide = 512
    keep = pl.pallas_call(
        rest_kernel,
        grid=(COLS // wide,),
        out_shape=jax.ShapeDtypeStruct((ROWS, PART), jnp.float32),
        in_specs=[
            pl.BlockSpec((1, BELIEFS), lambda t: (0, 0)),
            pl.BlockSpec((2, PART, wide), lambda t: (0, 0, t)),
            pl.BlockSpec((ACTS * ROWS, wide), lambda t: (0, t)),
            pl.BlockSpec((ACTS * ROWS, wide), lambda t: (0, t)),
        ],
        out_specs=pl.BlockSpec((ROWS, PART), lambda t: (0, 0)),
        scratch_shapes=[pltpu.VMEM((ACTS * ROWS, PART), jnp.float32)],
        compiler_params=pltpu.CompilerParams(vmem_limit_bytes=62 * 2**20),
        cost_estimate=pl.CostEstimate(flops=4 * 10**9, bytes_accessed=17 * 10**6, transcendentals=0),
        name="rest",
    )(owner, mixed, transitions, transitions2)
    summed = keep + got.astype(jnp.float32)
    row_action = lax.dynamic_slice_in_dim(action, (2 * high + core) * PART, PART)
    picked = (row_action[:, None] == jnp.arange(ACTS, dtype=jnp.int32)[None, :]).astype(jnp.bfloat16)
    gained = jnp.dot(picked, reward, preferred_element_type=jnp.float32)
    return (gained + DISCOUNT / S * summed.T).astype(jnp.bfloat16)


def solution(mesh):
    torus = Mesh(mesh.devices.reshape(8, 4, 2, 2, 2), ("z", "x", "yl", "yh", "co"))
    st = ("yh", "co")
    in_specs = (
        P(None, st),
        P(None, BEL, st),
        P(None, None, st),
        P(None, BEL),
        P(BEL, None, None),
        P(),
    )
    return jax.shard_map(body, mesh=torus, in_specs=in_specs, out_specs=P(st, BEL), check_vma=False)
```

```python
import jax
import jax.numpy as jnp
from jax import lax
from jax.experimental import pallas as pl
from jax.experimental.pallas import tpu as pltpu
from jax.sharding import Mesh
from jax.sharding import PartitionSpec as P

S = 12288
ACTS = 6
OBS = 48
ALPHAS = 512
BELIEFS = 1024
BEL = ("z", "x", "yl")
PEERS = 64
OWN = BELIEFS // PEERS
COLS = 3072
ROWS = 192
HALF = COLS // 128
LINES = 2 * HALF
PITCH = 64
GAP = 56
PART = 256
WEIGHTS = ALPHAS * PITCH
TOTAL = WEIGHTS + ACTS * OBS * LINES
STAGE = 32
DISCOUNT = 0.95

NT = (((1,), (1,)), ((), ()))


def choose_kernel(index_ref, action_ref, out_ref, row_ref):
    bel = (lax.axis_index("z") * 4 + lax.axis_index("x")) * 2 + lax.axis_index("yl")
    row_ref[...] = jnp.zeros_like(row_ref)
    for r in range(OWN):
        row_ref[r : r + 1, :OBS] = index_ref[action_ref[bel * OWN + r], r : r + 1, :]
    packed = row_ref[:8] + pltpu.roll(row_ref[8:], 64, axis=1)
    out_ref[...] = jnp.broadcast_to(packed[None], (PEERS, 8, 128))


def prep_kernel(
    alphas_ref, alphas2_ref, observe_ref, observe2_ref, lines_ref, rows_in, obs_in, wide_ref, out_ref, in_sems, out_sems
):
    parts = (
        ((alphas_ref, alphas2_ref), rows_in, ALPHAS // STAGE, 0, 0, PITCH),
        ((observe_ref, observe2_ref), obs_in, ACTS * OBS // STAGE, ALPHAS // STAGE, WEIGHTS, LINES),
    )

    def copy_in(part, t, s):
        sources, dest, _, at, _, _ = part
        here = pl.ds(pl.multiple_of(t * STAGE, STAGE), STAGE)
        return pltpu.make_async_copy(sources[s].at[here, :], dest.at[s, here, :], in_sems.at[at + t, s])

    def copy_out(part, t):
        _, _, _, at, first, pitch = part
        here = pl.ds(pl.multiple_of(first + t * STAGE * pitch, 16), STAGE * pitch)
        return pltpu.make_async_copy(out_ref.at[here, :], lines_ref.at[here, :], out_sems.at[at + t])

    for part in parts:

        def begin(t, _, part=part):
            for s in range(2):
                copy_in(part, t, s).start()
            return 0

        lax.fori_loop(0, part[2], begin, 0)
    for part in parts:

        def step(t, _, part=part):
            _, staged, _, _, first, pitch = part
            for s in range(2):
                copy_in(part, t, s).wait()
            for g in range(STAGE // 16):
                here = pl.ds(pl.multiple_of(t * STAGE + g * 16, 16), 16)
                for s in range(2):
                    for j in range(HALF):
                        got = staged[s, here, j * 128 : (j + 1) * 128]
                        wide_ref[g, pl.ds(s * HALF + j, 16, stride=GAP), :] = got.astype(jnp.float32)
                for r in range(16):
                    at = pl.multiple_of(first + (t * STAGE + g * 16 + r) * pitch, 16)
                    out_ref[pl.ds(at, LINES), :] = wide_ref[g, r * GAP : r * GAP + LINES, :].astype(jnp.bfloat16)
            copy_out(part, t).start()
            return 0

        lax.fori_loop(0, part[2], step, 0)
    for part in parts:

        def finish(t, _, part=part):
            copy_out(part, t).wait()
            return 0

        lax.fori_loop(0, part[2], finish, 0)


def pick(owner, got):
    value = got[:ROWS]
    for a in range(1, ACTS):
        value = jnp.where(owner == a, got[a * ROWS : (a + 1) * ROWS], value)
    return value


def main_kernel(
    index_ref, action_ref, owner_ref, source_ref, here_ref, there_ref,
    send_ref, mixed_ref, mixed2_ref, lines_ref, index_smem, weights_ref, mix_ref, block_ref, weight_sems, index_sem, lines_sem, mixed_sem,
):
    fetch = [
        pltpu.make_async_copy(source, weights_ref.at[n], weight_sems.at[n])
        for n, source in enumerate((here_ref, there_ref))
    ]
    lines = pltpu.make_async_copy(source_ref, lines_ref, lines_sem)
    table = pltpu.make_async_copy(index_ref, index_smem, index_sem)
    lines.start()
    table.start()
    for copy in fetch:
        copy.start()
    table.wait()
    lines.wait()
    rows_ref = lines_ref.at[pl.ds(0, WEIGHTS), :].reshape(ALPHAS, PITCH, 128)
    obs_ref = lines_ref.at[pl.ds(WEIGHTS, ACTS * OBS * LINES), :].reshape(ACTS * OBS, LINES, 128)
    high = lax.axis_index("yh")
    core = lax.axis_index("co")

    def sixteen(n, _):
        t = n // 16
        i = lax.rem(n, 16)
        source = (2 * jnp.where(t == 0, 1 - high, high) + core) * 16 + i
        for h in range(2):
            for r in range(8):
                a = action_ref[source * 16 + h * 8 + r]
                own = index_smem.at[source, r]
                weight = obs_ref.at[pl.ds(a * OBS, OBS)]
                total = None
                for o in range(OBS):
                    term = rows_ref[own[h * 64 + o], :LINES, :].astype(jnp.float32) * weight[o].astype(jnp.float32)
                    total = term if o == 0 else total + term
                mix_ref[(h * 8 + r) * GAP : (h * 8 + r) * GAP + LINES, :] = total
        for j in range(LINES):
            part = mix_ref[pl.ds(j, 16, stride=GAP), :]
            at = pl.ds(pl.multiple_of(i * 16, 16), 16)
            block_ref[t, j // HALF, at, (j % HALF) * 128 : (j % HALF + 1) * 128] = part.astype(jnp.bfloat16)
        return 0

    lax.fori_loop(0, 2 * PART // 16, sixteen, 0)
    mixed = [
        pltpu.make_async_copy(block_ref.at[1, n], out, mixed_sem.at[n]) for n, out in enumerate((mixed_ref, mixed2_ref))
    ]
    for copy in mixed:
        copy.start()
    for copy in fetch:
        copy.wait()
    got = lax.dot_general(weights_ref[0], block_ref[0, 0], NT, preferred_element_type=jnp.float32)
    got += lax.dot_general(weights_ref[1], block_ref[0, 1], NT, preferred_element_type=jnp.float32)
    first = pl.multiple_of((2 * (1 - high) + core) * PART, 128)
    send_ref[...] = pick(owner_ref[:, pl.ds(first, PART)], got).astype(send_ref.dtype)
    for copy in mixed:
        copy.wait()


def vmem():
    return pl.BlockSpec(memory_space=pltpu.VMEM)


def smem():
    return pl.BlockSpec(memory_space=pltpu.SMEM)


def hbm():
    return pl.BlockSpec(memory_space=pltpu.HBM)


def gather_blocks(packed):
    return lax.all_to_all(packed, BEL, 0, 0, tiled=True)


def body(alphas, transitions, observe, reward, belief_index, action):
    core = lax.axis_index("co")
    high = lax.axis_index("yh")
    across = [(0, 1), (1, 0)]
    observe = observe.reshape(ACTS * OBS, COLS)
    transitions = transitions.reshape(ACTS * ROWS, COLS)
    alphas2 = lax.ppermute(alphas, "co", across)
    observe2 = lax.ppermute(observe, "co", across)
    packed = pl.pallas_call(
        choose_kernel,
        out_shape=jax.ShapeDtypeStruct((PEERS, 8, 128), jnp.int32),
        in_specs=[vmem(), smem()],
        out_specs=vmem(),
        scratch_shapes=[pltpu.VMEM((OWN, 128), jnp.int32)],
        name="choose",
    )(belief_index.transpose(1, 0, 2), action)
    index = gather_blocks(packed)
    transitions2 = lax.ppermute(transitions, "co", across)
    lines = pl.pallas_call(
        prep_kernel,
        out_shape=jax.ShapeDtypeStruct((TOTAL, 128), jnp.bfloat16),
        in_specs=[hbm()] * 4,
        out_specs=hbm(),
        scratch_shapes=[
            pltpu.VMEM((2, ALPHAS, COLS), jnp.bfloat16),
            pltpu.VMEM((2, ACTS * OBS, COLS), jnp.bfloat16),
            pltpu.VMEM((STAGE // 16, 16 * GAP, 128), jnp.float32),
            pltpu.VMEM((TOTAL, 128), jnp.bfloat16),
            pltpu.SemaphoreType.DMA(((ALPHAS + ACTS * OBS) // STAGE, 2)),
            pltpu.SemaphoreType.DMA(((ALPHAS + ACTS * OBS) // STAGE,)),
        ],
        compiler_params=pltpu.CompilerParams(vmem_limit_bytes=62 * 2**20),
        cost_estimate=pl.CostEstimate(flops=8 * 10**9, bytes_accessed=10**7, transcendentals=0),
        name="prep",
    )(alphas, alphas2, observe, observe2)
    owner = action.reshape(1, BELIEFS)
    send, mixed, mixed2 = pl.pallas_call(
        main_kernel,
        out_shape=(
            jax.ShapeDtypeStruct((ROWS, PART), jnp.bfloat16),
            jax.ShapeDtypeStruct((PART, COLS), jnp.bfloat16),
            jax.ShapeDtypeStruct((PART, COLS), jnp.bfloat16),
        ),
        in_specs=[vmem(), smem(), vmem(), hbm(), hbm(), hbm()],
        out_specs=(vmem(), hbm(), hbm()),
        scratch_shapes=[
            pltpu.VMEM((TOTAL, 128), jnp.bfloat16),
            pltpu.SMEM((PEERS, 8, 128), jnp.int32),
            pltpu.VMEM((2, ACTS * ROWS, COLS), jnp.bfloat16),
            pltpu.VMEM((16 * GAP, 128), jnp.float32),
            pltpu.VMEM((2, 2, PART, COLS), jnp.bfloat16),
            pltpu.SemaphoreType.DMA((2,)),
            pltpu.SemaphoreType.DMA,
            pltpu.SemaphoreType.DMA,
            pltpu.SemaphoreType.DMA((2,)),
        ],
        compiler_params=pltpu.CompilerParams(vmem_limit_bytes=62 * 2**20),
        name="mix",
    )(index, action, owner, lines, transitions, transitions2)
    got = lax.ppermute(send, "yh", across)
    carried = lax.dot_general(transitions, mixed, NT, preferred_element_type=jnp.float32)
    carried += lax.dot_general(transitions2, mixed2, NT, preferred_element_type=jnp.float32)
    summed = pick(lax.dynamic_slice_in_dim(owner, (2 * high + core) * PART, PART, 1), carried) + got.astype(jnp.float32)
    row_action = lax.dynamic_slice_in_dim(action, (2 * high + core) * PART, PART)
    picked = (row_action[:, None] == jnp.arange(ACTS, dtype=jnp.int32)[None, :]).astype(jnp.bfloat16)
    gained = jnp.dot(picked, reward, preferred_element_type=jnp.float32)
    return (gained + DISCOUNT / S * summed.T).astype(jnp.bfloat16)


def solution(mesh):
    torus = Mesh(mesh.devices.reshape(8, 4, 2, 2, 2), ("z", "x", "yl", "yh", "co"))
    st = ("yh", "co")
    in_specs = (
        P(None, st),
        P(None, BEL, st),
        P(None, None, st),
        P(None, BEL),
        P(BEL, None, None),
        P(),
    )
    return jax.shard_map(body, mesh=torus, in_specs=in_specs, out_specs=P(st, BEL), check_vma=False)
```

```python
import jax
import jax.numpy as jnp
from jax import lax
from jax.experimental import pallas as pl
from jax.experimental.pallas import tpu as pltpu
from jax.sharding import Mesh
from jax.sharding import PartitionSpec as P

S = 12288
ACTS = 6
OBS = 48
ALPHAS = 512
BELIEFS = 1024
BEL = ("z", "x", "yl")
PEERS = 64
OWN = BELIEFS // PEERS
COLS = 3072
ROWS = 192
HALF = COLS // 128
LINES = 2 * HALF
PITCH = 64
GAP = 56
ODD = 49
PART = 256
WEIGHTS = ALPHAS * PITCH
TOTAL = WEIGHTS + ACTS * OBS * LINES
STAGE = 32
DISCOUNT = 0.95

NT = (((1,), (1,)), ((), ()))


def choose_kernel(index_ref, action_ref, out_ref, row_ref):
    bel = (lax.axis_index("z") * 4 + lax.axis_index("x")) * 2 + lax.axis_index("yl")
    row_ref[...] = jnp.zeros_like(row_ref)
    for r in range(OWN):
        row_ref[r : r + 1, :OBS] = index_ref[action_ref[bel * OWN + r], r : r + 1, :]
    packed = row_ref[:8] + pltpu.roll(row_ref[8:], 64, axis=1)
    out_ref[...] = jnp.broadcast_to(packed[None], (PEERS, 8, 128))


def prep_kernel(
    alphas_ref, alphas2_ref, observe_ref, observe2_ref, lines_ref, rows_in, obs_in, wide_ref, out_ref, in_sems, out_sems
):
    parts = (
        ((alphas_ref, alphas2_ref), rows_in, ALPHAS // STAGE, 0, 0, PITCH),
        ((observe_ref, observe2_ref), obs_in, ACTS * OBS // STAGE, ALPHAS // STAGE, WEIGHTS, LINES),
    )

    def copy_in(part, t, s):
        sources, dest, _, at, _, _ = part
        here = pl.ds(pl.multiple_of(t * STAGE, STAGE), STAGE)
        return pltpu.make_async_copy(sources[s].at[here, :], dest.at[s, here, :], in_sems.at[at + t, s])

    def copy_out(part, t):
        _, _, _, at, first, pitch = part
        here = pl.ds(pl.multiple_of(first + t * STAGE * pitch, 16), STAGE * pitch)
        return pltpu.make_async_copy(out_ref.at[here, :], lines_ref.at[here, :], out_sems.at[at + t])

    for part in parts:

        def begin(t, _, part=part):
            for s in range(2):
                copy_in(part, t, s).start()
            return 0

        lax.fori_loop(0, part[2], begin, 0)
    for part in parts:

        def step(t, _, part=part):
            _, staged, _, _, first, pitch = part
            for s in range(2):
                copy_in(part, t, s).wait()
            for g in range(STAGE // 16):
                here = pl.ds(pl.multiple_of(t * STAGE + g * 16, 16), 16)
                for s in range(2):
                    for j in range(HALF):
                        got = staged[s, here, j * 128 : (j + 1) * 128]
                        wide_ref[g, pl.ds(s * HALF + j, 16, stride=GAP), :] = got.astype(jnp.float32)
                for r in range(16):
                    at = pl.multiple_of(first + (t * STAGE + g * 16 + r) * pitch, 16)
                    out_ref[pl.ds(at, LINES), :] = wide_ref[g, r * GAP : r * GAP + LINES, :].astype(jnp.bfloat16)
            copy_out(part, t).start()
            return 0

        lax.fori_loop(0, part[2], step, 0)
    for part in parts:

        def finish(t, _, part=part):
            copy_out(part, t).wait()
            return 0

        lax.fori_loop(0, part[2], finish, 0)


def pick(owner, got):
    value = got[:ROWS]
    for a in range(1, ACTS):
        value = jnp.where(owner == a, got[a * ROWS : (a + 1) * ROWS], value)
    return value


def main_kernel(
    index_ref, action_ref, owner_ref, source_ref, here_ref, there_ref,
    send_ref, keep_ref, lines_ref, index_smem, weights_ref, mix_ref, block_ref, weight_sems, index_sems, lines_sem,
):
    fetch = [
        pltpu.make_async_copy(source, weights_ref.at[n], weight_sems.at[n])
        for n, source in enumerate((here_ref, there_ref))
    ]
    lines = pltpu.make_async_copy(source_ref, lines_ref, lines_sem)
    high = lax.axis_index("yh")
    core = lax.axis_index("co")
    tables = []
    for t, yh in enumerate((1 - high, high)):
        source = pl.ds((2 * yh + core) * 16, 16)
        tables.append(pltpu.make_async_copy(index_ref.at[source], index_smem.at[source], index_sems.at[t]))
    tables[0].start()
    lines.start()
    tables[1].start()
    for copy in fetch:
        copy.start()
    for copy in tables:
        copy.wait()
    lines.wait()
    rows_ref = lines_ref.at[pl.ds(0, WEIGHTS), :].reshape(ALPHAS, PITCH, 128)
    obs_ref = lines_ref.at[pl.ds(WEIGHTS, ACTS * OBS * LINES), :].reshape(ACTS * OBS, LINES, 128)

    def sixteen(n, _):
        t = n // 16
        i = lax.rem(n, 16)
        source = (2 * jnp.where(t == 0, 1 - high, high) + core) * 16 + i
        for h in range(2):
            for r in range(8):
                a = action_ref[source * 16 + h * 8 + r]
                weight = obs_ref.at[pl.ds(a * OBS, OBS)]
                total = None
                for o in range(OBS):
                    term = rows_ref[index_smem[source, r, h * 64 + o], :LINES, :].astype(jnp.float32) * weight[o].astype(jnp.float32)
                    total = term if o == 0 else total + term
                mix_ref[(h * 8 + r) * ODD : (h * 8 + r) * ODD + LINES, :] = total
        for j in range(LINES):
            part = mix_ref[pl.ds(j, 16, stride=ODD), :]
            at = pl.ds(pl.multiple_of(i * 16, 16), 16)
            block_ref[t, j // HALF, at, (j % HALF) * 128 : (j % HALF + 1) * 128] = part.astype(jnp.bfloat16)
        return 0

    lax.fori_loop(0, 2 * PART // 16, sixteen, 0)
    for copy in fetch:
        copy.wait()

    def product(t, _):
        got = lax.dot_general(weights_ref[0], block_ref[t, 0], NT, preferred_element_type=jnp.float32)
        got += lax.dot_general(weights_ref[1], block_ref[t, 1], NT, preferred_element_type=jnp.float32)
        first = pl.multiple_of((2 * jnp.where(t == 0, 1 - high, high) + core) * PART, 128)
        value = pick(owner_ref[:, pl.ds(first, PART)], got)

        @pl.when(t == 0)
        def _():
            send_ref[...] = value.astype(send_ref.dtype)

        @pl.when(t == 1)
        def _():
            keep_ref[...] = value

        return 0

    lax.fori_loop(0, 2, product, 0)


def vmem():
    return pl.BlockSpec(memory_space=pltpu.VMEM)


def smem():
    return pl.BlockSpec(memory_space=pltpu.SMEM)


def hbm():
    return pl.BlockSpec(memory_space=pltpu.HBM)


def gather_blocks(packed):
    return lax.all_to_all(packed, BEL, 0, 0, tiled=True)


def body(alphas, transitions, observe, reward, belief_index, action):
    core = lax.axis_index("co")
    high = lax.axis_index("yh")
    across = [(0, 1), (1, 0)]
    observe = observe.reshape(ACTS * OBS, COLS)
    transitions = transitions.reshape(ACTS * ROWS, COLS)
    alphas2 = lax.ppermute(alphas, "co", across)
    observe2 = lax.ppermute(observe, "co", across)
    packed = pl.pallas_call(
        choose_kernel,
        out_shape=jax.ShapeDtypeStruct((PEERS, 8, 128), jnp.int32),
        in_specs=[vmem(), smem()],
        out_specs=vmem(),
        scratch_shapes=[pltpu.VMEM((OWN, 128), jnp.int32)],
        name="choose",
    )(belief_index.transpose(1, 0, 2), action)
    index = gather_blocks(packed)
    transitions2 = lax.ppermute(transitions, "co", across)
    lines = pl.pallas_call(
        prep_kernel,
        out_shape=jax.ShapeDtypeStruct((TOTAL, 128), jnp.bfloat16),
        in_specs=[hbm()] * 4,
        out_specs=hbm(),
        scratch_shapes=[
            pltpu.VMEM((2, ALPHAS, COLS), jnp.bfloat16),
            pltpu.VMEM((2, ACTS * OBS, COLS), jnp.bfloat16),
            pltpu.VMEM((STAGE // 16, 16 * GAP, 128), jnp.float32),
            pltpu.VMEM((TOTAL, 128), jnp.bfloat16),
            pltpu.SemaphoreType.DMA(((ALPHAS + ACTS * OBS) // STAGE, 2)),
            pltpu.SemaphoreType.DMA(((ALPHAS + ACTS * OBS) // STAGE,)),
        ],
        compiler_params=pltpu.CompilerParams(vmem_limit_bytes=62 * 2**20),
        cost_estimate=pl.CostEstimate(flops=8 * 10**9, bytes_accessed=10**7, transcendentals=0),
        name="prep",
    )(alphas, alphas2, observe, observe2)
    owner = action.reshape(1, BELIEFS)
    send, keep = pl.pallas_call(
        main_kernel,
        out_shape=(
            jax.ShapeDtypeStruct((ROWS, PART), jnp.bfloat16),
            jax.ShapeDtypeStruct((ROWS, PART), jnp.float32),
        ),
        in_specs=[hbm(), smem(), vmem(), hbm(), hbm(), hbm()],
        out_specs=(vmem(), vmem()),
        scratch_shapes=[
            pltpu.VMEM((TOTAL, 128), jnp.bfloat16),
            pltpu.SMEM((PEERS, 8, 128), jnp.int32),
            pltpu.VMEM((2, ACTS * ROWS, COLS), jnp.bfloat16),
            pltpu.VMEM((16 * ODD, 128), jnp.float32),
            pltpu.VMEM((2, 2, PART, COLS), jnp.bfloat16),
            pltpu.SemaphoreType.DMA((2,)),
            pltpu.SemaphoreType.DMA((2,)),
            pltpu.SemaphoreType.DMA,
        ],
        compiler_params=pltpu.CompilerParams(vmem_limit_bytes=62 * 2**20),
        name="mix",
    )(index, action, owner, lines, transitions, transitions2)
    got = lax.ppermute(send, "yh", across)
    summed = keep + got.astype(jnp.float32)
    row_action = lax.dynamic_slice_in_dim(action, (2 * high + core) * PART, PART)
    picked = (row_action[:, None] == jnp.arange(ACTS, dtype=jnp.int32)[None, :]).astype(jnp.bfloat16)
    gained = jnp.dot(picked, reward, preferred_element_type=jnp.float32)
    return (gained + DISCOUNT / S * summed.T).astype(jnp.bfloat16)


def solution(mesh):
    torus = Mesh(mesh.devices.reshape(8, 4, 2, 2, 2), ("z", "x", "yl", "yh", "co"))
    st = ("yh", "co")
    in_specs = (
        P(None, st),
        P(None, BEL, st),
        P(None, None, st),
        P(None, BEL),
        P(BEL, None, None),
        P(),
    )
    return jax.shard_map(body, mesh=torus, in_specs=in_specs, out_specs=P(st, BEL), check_vma=False)
```
